32 devices in a mesh: seq: 8 (over y, x, core), dp: 4 (over z).
Axes of the slice: x: 2, y: 2, z: 4, core: 2. Of those that a mesh axis runs over, the one named last changes fastest.
Arguments:
- teacher_video: bfloat16 [4, 3, 1024, 1536], P('dp', None, 'seq'), may hold values from -150 to 150
- student_video: bfloat16 [4, 3, 1024, 1536], P('dp', None, 'seq'), may hold values from -150 to 150
- teacher_audio: bfloat16 [4, 2, 256, 1536], P('dp', None, 'seq'), may hold values from -5 to 5
- student_audio: bfloat16 [4, 2, 256, 1536], P('dp', None, 'seq'), may hold values from -5 to 5
- alignment: int32 [4, 8, 2], P('dp', 'seq'), may hold values from 0 to 7, as said below
- guidance_index: int32 [4], P('dp'), may hold values from 0 to 7
- step_index: int32 [4], P('dp'), may hold values from 0 to 999
- null_flag: int32 [4], P('dp'), may hold values from 0 to 1, as said below
- gamma: float32 [8, 12], replicated, may hold values from -0.5 to 0.5
Outputs:
- grad_video: bfloat16 [4, 3, 1024, 1536], P('dp', None, 'seq')
- grad_audio: bfloat16 [4, 2, 256, 1536], P('dp', None, 'seq')
- gamma_grad: float32 [8, 12], replicated
The draws below stay inside these ranges and needn't reach their ends.
Inputs may be any that keep to these rules, and one draw needn't show every extreme that they name: For video block i, alignment[b, i] holds the first audio block s and the number c >= 1 of consecutive audio blocks that intersect it in time; blocks s to s + c - 1 lie inside the clip and within 3 blocks of audio block i. `null_flag`: at least one clip is dropped and at least one is kept.
All inputs are finite; a program needn't handle non-finite values.
Results may differ from the reference program's by a relative error of at most 0.013.
Values may be sent and summed in bfloat16 or wider, within the bound.
A program may use at most 64 MiB of HBM per device.

```python
import jax
import jax.numpy as jnp
from jax import lax

HEADS = 12
HEAD_DIM = 128
TV = 128
TA = 32
VB = 128
REACH = 3
GLEVELS = 8
CLIPS = 4
NV = 1024
NA = 256
NVB = 8


def video_draw(key):
    feature_width = HEADS * HEAD_DIM
    shape = (CLIPS, NV, feature_width)
    pieces = jax.random.split(key, 3)
    query = jnp.clip(jax.random.normal(pieces[0], shape, jnp.float32), -5.0, 5.0)
    keys_drawn = jnp.clip(jax.random.normal(pieces[1], shape, jnp.float32), -5.0, 5.0)
    values = jnp.clip(jax.random.normal(pieces[2], shape, jnp.float32), -5.0, 5.0)
    return jnp.clip(jnp.stack([query, keys_drawn, values], axis=1), -150.0, 150.0).astype(jnp.bfloat16)


def draw_teacher_video(key, part):
    return video_draw(jax.random.fold_in(key, 11))


def draw_student_video(key, part):
    return video_draw(jax.random.fold_in(key, 23))


def draw_alignment(key, part):
    owners = NV // TV
    per_device = TV // VB
    blocks = jnp.arange(NVB, dtype=jnp.int32)
    center = blocks // per_device
    low_edge = jnp.maximum(0, center - REACH)
    high_edge = jnp.minimum(owners - 1, center + REACH)
    avail = high_edge - low_edge + 1
    random_ints = jax.random.randint(jax.random.fold_in(key, 37), (CLIPS, NVB, 2), 0, 840, jnp.int32)
    block_count = 1 + random_ints[..., 0] % avail
    block_count = jnp.where(blocks % 16 == 0, avail, block_count)
    first_block = low_edge + random_ints[..., 1] % (avail - block_count + 1)
    return jnp.stack([first_block, block_count], axis=-1).astype(jnp.int32)


def draw_null_flag(key, part):
    pieces = jax.random.split(jax.random.fold_in(key, 53), 2)
    flags = jax.random.randint(pieces[0], (CLIPS,), 0, 2, jnp.int32)
    chosen = jax.random.randint(pieces[1], (), 0, CLIPS, jnp.int32)
    slots = jnp.arange(CLIPS, dtype=jnp.int32)
    flags = jnp.where(slots == chosen, 1, flags)
    flags = jnp.where(slots == (chosen + 1) % CLIPS, 0, flags)
    return flags.astype(jnp.int32)


def plant(values, key, least, largest):
    index_at = [jax.random.randint(jax.random.fold_in(key, axis), (), 0, length) for axis, length in enumerate(values.shape)]
    widest = values.shape.index(max(values.shape))
    beside = index_at[:widest] + [(index_at[widest] + 1) % values.shape[widest]] + index_at[widest + 1:]
    return values.at[tuple(index_at)].set(least).at[tuple(beside)].set(largest)


def shard_levels(rng, dims, cuts, low, high):
    gain = 1.0
    for axis_at, blocks in cuts:
        draws = jax.random.uniform(jax.random.fold_in(jax.random.fold_in(rng, 6), axis_at), (blocks,), jnp.float32, low / len(cuts), high / len(cuts))
        gain = gain * jnp.repeat(jnp.exp(draws), dims[axis_at] // blocks).reshape((-1,) + (1,) * (len(dims) - 1 - axis_at))
    return gain


def gaussian(own_key, extent, deviation, limit, shards=(), kind=jnp.bfloat16):
    result = jax.random.normal(own_key, extent, jnp.float32) * deviation
    if len(shards) > 0:
        result = shard_levels(own_key, extent, shards, -0.22, 0.18) * result
    return jnp.clip(result, min=-limit, max=limit).astype(kind)


def setup_inputs(seed: int = 0) -> dict:
    splits = jax.random.split(jax.random.key(seed), 10)
    return {
        "teacher_video": draw_teacher_video(jax.random.fold_in(splits[9], 71), 0),
        "student_video": draw_student_video(jax.random.fold_in(splits[9], 71), 0),
        "teacher_audio": gaussian(splits[2], (CLIPS, 2, NA, HEADS * HEAD_DIM), 1.0, 5.0, ((0, 4), (2, 8))),
        "student_audio": gaussian(splits[3], (CLIPS, 2, NA, HEADS * HEAD_DIM), 1.0, 5.0, ((0, 4), (2, 8))),
        "alignment": draw_alignment(jax.random.fold_in(splits[9], 71), 0),
        "guidance_index": plant(jax.random.randint(splits[5], (CLIPS,), 0, GLEVELS), jax.random.fold_in(splits[5], 1), 0, GLEVELS - 1).astype(jnp.int32),
        "step_index": plant(jax.random.randint(splits[6], (CLIPS,), 0, 1000), jax.random.fold_in(splits[6], 1), 0, 999).astype(jnp.int32),
        "null_flag": draw_null_flag(jax.random.fold_in(splits[9], 71), 0),
        "gamma": jnp.clip(jax.random.uniform(splits[8], (GLEVELS, HEADS), jnp.float32, -0.5, 0.5), -0.5, 0.5),
    }


def as_float(array):
    return array.astype(jnp.float32)


def joint_probs(scores, usable):
    masked = jnp.where(usable, scores, -jnp.inf)
    highest = jnp.max(masked, axis=-1, keepdims=True)
    exponent = jnp.exp(masked - highest)
    return exponent / jnp.sum(exponent, axis=-1, keepdims=True)


def reference(teacher_video, student_video, teacher_audio, student_audio, alignment, guidance_index, step_index, null_flag, gamma):
    feature_width = HEADS * HEAD_DIM
    window = (2 * REACH + 1) * TA
    score_scale = HEAD_DIM ** -0.5
    levels = jnp.arange(GLEVELS, dtype=jnp.int32)
    video_list = []
    audio_list = []
    gamma_total = jnp.zeros((GLEVELS, HEADS), jnp.float32)
    for clip_index in range(CLIPS):
        level_index = guidance_index[clip_index]
        weight = 1.0 + 0.75 * level_index.astype(jnp.float32)
        loss_weight = 1.0 / (1.0 + step_index[clip_index].astype(jnp.float32) / 250.0)
        keep_audio = null_flag[clip_index] == 0
        factor = jnp.sum(jnp.where(levels[:, None] == level_index, gamma, jnp.zeros_like(gamma)), axis=0)
        teacher_pad = jnp.pad(teacher_audio[clip_index], ((0, 0), (0, window), (0, 0)))
        student_pad = jnp.pad(student_audio[clip_index], ((0, 0), (0, window), (0, 0)))
        teach_clip = teacher_video[clip_index]
        pupil_clip = student_video[clip_index]

        def advance(carried, block_index):
            audio_sums, head_totals = carried
            first_block = alignment[clip_index, block_index, 0].astype(jnp.int32)
            block_count = alignment[clip_index, block_index, 1].astype(jnp.int32)
            offset = (block_index * VB).astype(jnp.int32)
            teach_vid = lax.dynamic_slice_in_dim(teach_clip, offset, VB, 1).reshape(3, VB, HEADS, HEAD_DIM)
            pupil_vid = lax.dynamic_slice_in_dim(pupil_clip, offset, VB, 1).reshape(3, VB, HEADS, HEAD_DIM)
            low_edge = (first_block * TA).astype(jnp.int32)
            teach_aud = lax.dynamic_slice_in_dim(teacher_pad, low_edge, window, 1).reshape(2, window, HEADS, HEAD_DIM)
            pupil_aud = lax.dynamic_slice_in_dim(student_pad, low_edge, window, 1).reshape(2, window, HEADS, HEAD_DIM)
            audio_ok = ((jnp.arange(window, dtype=jnp.int32) // TA) < block_count) & keep_audio
            usable = jnp.concatenate([jnp.ones((VB,), bool), audio_ok])[None, None, :]
            teach_keys = jnp.concatenate([teach_vid[1], teach_aud[0]], axis=0)
            teach_values = jnp.concatenate([teach_vid[2], teach_aud[1]], axis=0)
            teach_scores = jnp.einsum("qhe,khe->hqk", as_float(teach_vid[0]), as_float(teach_keys)) * score_scale
            cond_probs = joint_probs(teach_scores, usable).astype(jnp.bfloat16)
            conditional = jnp.einsum("hqk,khe->qhe", as_float(cond_probs), as_float(teach_values))
            plain_probs = joint_probs(teach_scores[..., :VB], jnp.ones((1, 1, VB), bool)).astype(jnp.bfloat16)
            unconditional = jnp.einsum("hqk,khe->qhe", as_float(plain_probs), as_float(teach_vid[2]))
            target = unconditional + weight * (conditional - unconditional)
            pupil_query = pupil_vid[0]
            pupil_keys = jnp.concatenate([pupil_vid[1], pupil_aud[0]], axis=0)
            pupil_values = jnp.concatenate([pupil_vid[2], pupil_aud[1]], axis=0)
            pupil_scores = jnp.einsum("qhe,khe->hqk", as_float(pupil_query), as_float(pupil_keys)) * score_scale
            probs = joint_probs(pupil_scores, usable)
            probs_round = probs.astype(jnp.bfloat16)
            student_out = jnp.einsum("hqk,khe->qhe", as_float(probs_round), as_float(pupil_values))
            residual = loss_weight * (student_out * factor[None, :, None] - target)
            head_sums = jnp.sum(residual * student_out, axis=(0, 2))
            out_grad = (residual * factor[None, :, None]).astype(jnp.bfloat16)
            prob_grad = jnp.einsum("qhe,khe->hqk", as_float(out_grad), as_float(pupil_values))
            row_delta = jnp.sum(as_float(out_grad) * student_out, axis=-1)
            score_grad = (score_scale * probs * (prob_grad - jnp.transpose(row_delta)[:, :, None])).astype(jnp.bfloat16)
            query_grad = jnp.einsum("hqk,khe->qhe", as_float(score_grad), as_float(pupil_keys))
            key_grad = jnp.einsum("hqk,qhe->khe", as_float(score_grad), as_float(pupil_query))
            value_grad = jnp.einsum("hqk,qhe->khe", as_float(probs_round), as_float(out_grad))
            video_grad = jnp.stack([query_grad, key_grad[:VB], value_grad[:VB]]).reshape(3, VB, feature_width).astype(jnp.bfloat16)
            audio_grad = jnp.stack([key_grad[VB:], value_grad[VB:]]).reshape(2, window, feature_width)
            placed = lax.dynamic_slice_in_dim(audio_sums, low_edge, window, 1) + audio_grad
            audio_sums = lax.dynamic_update_slice_in_dim(audio_sums, placed, low_edge, 1)
            return (audio_sums, head_totals + head_sums), video_grad

        initial = (jnp.zeros((2, NA + window, feature_width), jnp.float32), jnp.zeros((HEADS,), jnp.float32))
        (audio_sums, head_totals), video_blocks = lax.scan(advance, initial, jnp.arange(NVB, dtype=jnp.int32))
        video_list.append(jnp.transpose(video_blocks, (1, 0, 2, 3)).reshape(3, NV, feature_width))
        audio_list.append(audio_sums[:, :NA].astype(jnp.bfloat16))
        gamma_total = gamma_total + jnp.where(levels[:, None] == level_index, head_totals[None, :], jnp.zeros_like(gamma_total))
    return jnp.stack(video_list), jnp.stack(audio_list), gamma_total / (NV * HEAD_DIM)
```

```python
import functools

import jax
import jax.numpy as jnp
from jax import lax
from jax.experimental import pallas as pl
from jax.experimental.pallas import tpu as pltpu
from jax.sharding import PartitionSpec as P

VB = 128
REACH = 3
SLOTS = 2 * REACH + 1
GROUPS = 4
MESH = pl.DeviceIdType.MESH
F32 = jnp.float32
BF16 = jnp.bfloat16


def dot(a, b, dims):
    return lax.dot_general(a, b, (dims, ((), ())), preferred_element_type=F32)


NT = ((1,), (1,))
NN = ((1,), (0,))
TN = ((0,), (0,))


def kernel(
    n, m, groups, heads,
    tv, sv, ta, sa, align, level_ref, step_ref, null_ref, gamma,
    gv_out, ga_out, gg_out,
    kv, qt, qs, gv, ga, pb, rp, rr, rd, ru, sdir, sind, suni, tot, gbuf, gbuf2, gout,
    load_sem, out_sem, in_send, in_recv, a_send, a_recv, g_send, g_recv, gam_send, gam_recv,
):
    width = tv.shape[-1]
    ta_len = ta.shape[2]
    hd = width // heads
    hpg = heads // groups
    gw = hpg * hd
    window = SLOTS * ta_len
    keys = VB + window
    scale = hd ** (-0.5)
    pairs = n // 2

    i = lax.axis_index("seq")
    z = lax.axis_index("dp")
    c = i % 2
    p = i // 2
    po = p % 2
    pe = 1 - po
    dirn = 1 - 2 * po
    d = 2 * c - 1
    partner = i - d
    lo_ok = i >= 2
    hi_ok = i + 2 < n
    ut = i + 3 * d
    u_ok = (ut >= 0) & (ut < n)
    u_slot = 6 * c
    relay = ((po == 0) & (p + 2 < pairs)) | ((po == 1) & (p >= 3))
    relay_direct = c == po
    relay_dev = i + 5 * pe - 1 - 3 * c
    ind_dev = i - 1 - 3 * pe + 5 * c
    ind_ok = ((po == 0) & lo_ok) | ((po == 1) & hi_ok)
    aff_dir = relay & relay_direct
    aff_uni = relay & jnp.logical_not(relay_direct)

    def krows(r):
        return pl.ds(pl.multiple_of(VB + ta_len * r, ta_len), ta_len)

    def prows(r):
        return pl.ds(pl.multiple_of(ta_len * r, ta_len), ta_len)

    def cols(g):
        return pl.ds(g * gw, gw)

    loads = [
        pltpu.make_async_copy(ta.at[0], kv.at[0:2, krows(REACH), :], load_sem.at[0]),
        pltpu.make_async_copy(sa.at[0], kv.at[2:4, krows(REACH), :], load_sem.at[1]),
        pltpu.make_async_copy(tv.at[0, 0], qt, load_sem.at[2]),
        pltpu.make_async_copy(tv.at[0, 1:3], kv.at[0:2, 0:VB, :], load_sem.at[3]),
        pltpu.make_async_copy(sv.at[0, 0], qs, load_sem.at[4]),
        pltpu.make_async_copy(sv.at[0, 1:3], kv.at[2:4, 0:VB, :], load_sem.at[5]),
    ]
    for load in loads:
        load.start()

    barrier = pltpu.get_barrier_semaphore()

    def greet_seq(k, carry):
        pl.semaphore_signal(barrier, inc=1, device_id={"seq": (i + k) % n}, device_id_type=MESH)
        return carry

    def greet_dp(k, carry):
        pl.semaphore_signal(barrier, inc=1, device_id={"dp": (z + k) % m}, device_id_type=MESH)
        return carry

    lax.fori_loop(1, n, greet_seq, 0)
    lax.fori_loop(1, m, greet_dp, 0)

    def clear(r):
        kv[:, krows(r), :] = jnp.zeros((4, ta_len, width), BF16)

    @pl.when(jnp.logical_not(lo_ok))
    def _():
        clear(1)
        clear(1 - d)

    @pl.when(jnp.logical_not(hi_ok))
    def _():
        clear(5)
        clear(5 - d)

    @pl.when(jnp.logical_not(u_ok))
    def _():
        clear(u_slot)
        ru[...] = jnp.zeros(ru.shape, BF16)

    tot[...] = jnp.zeros(tot.shape, F32)
    pl.semaphore_wait(barrier, (n - 1) + (m - 1))
    loads[0].wait()
    loads[1].wait()

    def in_copy(g, kind, src, dst, dev):
        return pltpu.make_async_remote_copy(
            src_ref=kv.at[:, krows(src), cols(g)],
            dst_ref=kv.at[:, krows(dst), cols(g)],
            send_sem=in_send.at[g, kind],
            recv_sem=in_recv.at[g, dst],
            device_id={"seq": dev},
            device_id_type=MESH,
        )

    def in_wait(g, r):
        ref = kv.at[:, krows(r), cols(g)]
        pltpu.make_async_copy(ref, ref, in_recv.at[g, r]).wait()

    relay_slot = jnp.where(relay_direct, 3 + 2 * dirn, u_slot)

    def in_sends(g):
        return (
            (in_copy(g, 0, REACH, 3 - 2 * dirn, i + 2 * dirn), None),
            (in_copy(g, 1, REACH, 3 - 3 * d, ut), u_ok),
            (in_copy(g, 2, REACH, 3 + d, partner), None),
            (in_copy(g, 3, relay_slot, 1 + 4 * c, relay_dev), relay),
            (in_copy(g, 4, 1, 1 + d, partner), lo_ok),
            (in_copy(g, 5, 5, 5 + d, partner), hi_ok),
        )

    def guarded(cond, act):
        if cond is None:
            act()
        else:
            pl.when(cond)(act)

    def own(g):
        for copy, cond in in_sends(g)[:3]:
            guarded(cond, copy.start)

    def forward(g):
        guarded(lo_ok, lambda: in_wait(g, 1))
        guarded(hi_ok, lambda: in_wait(g, 5))
        guarded(u_ok, lambda: in_wait(g, u_slot))
        for copy, cond in in_sends(g)[3:]:
            guarded(cond, copy.start)

    level = level_ref[0]
    weight = 1.0 + 0.75 * level.astype(F32)
    loss_weight = 1.0 / (1.0 + jnp.full((1, hd), step_ref[0], jnp.int32).astype(F32) / 250.0)
    first = align[0, 0, 0]
    count = align[0, 0, 1]
    keep = null_ref[0]
    kcol = lax.broadcasted_iota(jnp.int32, (VB, keys), 1)
    owner = i - REACH + (kcol - VB) // ta_len
    usable = (kcol < VB) | ((owner >= first) & (owner < first + count) & (keep == 0))

    def softmax(s):
        e = jnp.exp(s - jnp.max(s, axis=-1, keepdims=True))
        return e * (1.0 / jnp.sum(e, axis=-1, keepdims=True))

    def head(h):
        hc = pl.ds(h * hd, hd)
        k = kv[0, :, hc]
        v = kv[1, :, hc]
        s = dot(qt[:, hc], k, NT) * scale
        cond = dot(softmax(jnp.where(usable, s, -jnp.inf)).astype(BF16), v, NN)
        unc = dot(softmax(s[:, :VB]).astype(BF16), v[:VB], NN)
        target = unc + weight * (cond - unc)
        k = kv[2, :, hc]
        v = kv[3, :, hc]
        q = qs[:, hc]
        s = dot(q, k, NT) * scale
        probs = softmax(jnp.where(usable, s, -jnp.inf))
        pround = probs.astype(BF16)
        out = dot(pround, v, NN)
        factor = gamma[level, h]
        residual = loss_weight * (out * factor - target)
        tot[h : h + 1, :] = jnp.sum(residual * out, axis=0, keepdims=True)
        og = (residual * factor).astype(BF16)
        pg = dot(og, v, NT)
        delta = jnp.sum(og.astype(F32) * out, axis=-1, keepdims=True)
        sg = (scale * probs * (pg - delta)).astype(BF16)
        gv[0, :, hc] = dot(sg, k, NN).astype(BF16)
        kg = dot(sg, q, TN).astype(BF16)
        vg = dot(pround, og, TN).astype(BF16)
        gv[1, :, hc] = kg[:VB]
        gv[2, :, hc] = vg[:VB]
        pb[0, :, hc] = kg[VB:]
        pb[1, :, hc] = vg[VB:]

    def gv_copy(g):
        return pltpu.make_async_copy(gv.at[:, :, cols(g)], gv_out.at[0, :, :, cols(g)], out_sem.at[g])

    def compute(g):
        in_wait(g, 3 - d)
        guarded(lo_ok, lambda: in_wait(g, 1 - d))
        guarded(hi_ok, lambda: in_wait(g, 5 - d))
        if g == 0:
            for load in loads[2:]:
                load.wait()
        for h in range(g * hpg, (g + 1) * hpg):
            head(h)
        gv_copy(g).start()

    base = 1 - d

    def a_copies(g):
        return [
            pltpu.make_async_remote_copy(
                src_ref=pb.at[:, prows(base + 2 * k), cols(g)],
                dst_ref=rp.at[k, :, :, cols(g)],
                send_sem=a_send.at[g, k],
                recv_sem=a_recv.at[g, k],
                device_id={"seq": partner},
                device_id_type=MESH,
            )
            for k in range(3)
        ]

    def stage_a(g):
        for copy in a_copies(g):
            copy.start()

    def g_copy(g, kind, src, dst, dev):
        return pltpu.make_async_remote_copy(
            src_ref=src,
            dst_ref=dst.at[:, :, cols(g)],
            send_sem=g_send.at[g, kind],
            recv_sem=g_recv.at[g, kind],
            device_id={"seq": dev},
            device_id_type=MESH,
        )

    def dir_copy(g):
        return g_copy(g, 0, sdir.at[:, :, cols(g)], rd, i + 2 * dirn)

    def uni_copy(g):
        return g_copy(g, 1, suni.at[:, :, cols(g)], ru, ut)

    def uni_plain(g):
        return g_copy(g, 1, pb.at[:, prows(u_slot), cols(g)], ru, ut)

    def ind_copy(g):
        return g_copy(g, 2, sind.at[:, :, cols(g)], rr, ind_dev)

    def stage_b(g):
        for copy in a_copies(g):
            copy.wait_recv()
        cs = cols(g)

        @pl.when(ind_ok)
        def _():
            sind[:, :, cs] = (
                pb[:, prows(3 - 2 * dirn), cs].astype(F32) + rp[1 - dirn, :, :, cs].astype(F32)
            ).astype(BF16)
            ind_copy(g).start()

        pl.when(u_ok & jnp.logical_not(aff_uni))(uni_plain(g).start)

        @pl.when(jnp.logical_not(aff_dir))
        def _():
            sdir[:, :, cs] = (
                pb[:, prows(3 + 2 * dirn), cs].astype(F32) + rp[1 + dirn, :, :, cs].astype(F32)
            ).astype(BF16)
            dir_copy(g).start()

    def stage_c(g):
        cs = cols(g)
        pl.when(relay)(lambda: ind_copy(g).wait_recv())

        @pl.when(aff_dir)
        def _():
            sdir[:, :, cs] = (
                pb[:, prows(3 + 2 * dirn), cs].astype(F32)
                + rp[1 + dirn, :, :, cs].astype(F32)
                + rr[:, :, cs].astype(F32)
            ).astype(BF16)
            dir_copy(g).start()

        @pl.when(aff_uni)
        def _():
            suni[:, :, cs] = (
                pb[:, prows(u_slot), cs].astype(F32) + rr[:, :, cs].astype(F32)
            ).astype(BF16)
            uni_copy(g).start()

    def stage_d(g):
        cs = cols(g)
        dir_copy(g).wait_recv()
        pl.when(u_ok)(lambda: uni_copy(g).wait_recv())
        ga[:, :, cs] = (
            pb[:, prows(REACH), cs].astype(F32)
            + rp[1, :, :, cs].astype(F32)
            + rd[:, :, cs].astype(F32)
            + ru[:, :, cs].astype(F32)
        ).astype(BF16)

    def gam_exchange(buf, which, size, me, axis):
        def send(k, carry):
            pltpu.make_async_remote_copy(
                src_ref=buf.at[me],
                dst_ref=buf.at[me],
                send_sem=gam_send.at[which],
                recv_sem=gam_recv.at[which],
                device_id={axis: (me + k) % size},
                device_id_type=MESH,
            ).start()
            return carry

        lax.fori_loop(1, size, send, 0)

    def gam_wait(buf, which, size, sem):
        ref = buf.at[0 : size - 1]
        pltpu.make_async_copy(ref, ref, sem.at[which]).wait()

    def gamma_first():
        sums = jnp.sum(tot[...], axis=-1, keepdims=True)
        rows = lax.broadcasted_iota(jnp.int32, tot.shape, 0)
        lanes = lax.broadcasted_iota(jnp.int32, tot.shape, 1)
        vec = jnp.sum(jnp.where(rows == lanes, sums, 0.0), axis=0, keepdims=True)
        vec = vec / (VB * n * hd)
        levels = lax.broadcasted_iota(jnp.int32, gbuf.shape[1:], 0)
        gbuf[i] = jnp.where(levels == level, vec, 0.0)
        gam_exchange(gbuf, 0, n, i, "seq")

    def gamma_second():
        gam_wait(gbuf, 0, n, gam_recv)
        gbuf2[z] = jnp.sum(gbuf[...], axis=0)
        gam_exchange(gbuf2, 1, m, z, "dp")

    def gamma_last():
        gam_wait(gbuf2, 1, m, gam_recv)
        gout[...] = jnp.sum(gbuf2[...], axis=0)[:, : gout.shape[1]]

    own(0)
    for t in range(groups + 4):
        if t + 1 < groups:
            own(t + 1)
        if t < groups:
            forward(t)
        if 0 <= t - 1 < groups:
            compute(t - 1)
            stage_a(t - 1)
            if t - 1 == groups - 1:
                gamma_first()
        if 0 <= t - 2 < groups:
            stage_b(t - 2)
        if 0 <= t - 3 < groups:
            stage_c(t - 3)
        if t == groups + 2:
            gamma_second()
        if 0 <= t - 4 < groups:
            stage_d(t - 4)
    ga_copy = pltpu.make_async_copy(ga, ga_out.at[0], load_sem.at[0])
    ga_copy.start()
    gamma_last()
    gg_copy = pltpu.make_async_copy(gout, gg_out, load_sem.at[1])
    gg_copy.start()
    for g in range(groups):
        gv_copy(g).wait()
        for copy, cond in in_sends(g):
            guarded(cond, copy.wait_send)
        for copy in a_copies(g):
            copy.wait_send()
        dir_copy(g).wait_send()
        pl.when(u_ok)(lambda: uni_copy(g).wait_send())
        pl.when(ind_ok)(lambda: ind_copy(g).wait_send())
    gam_wait(gbuf, 0, n, gam_send)
    gam_wait(gbuf2, 1, m, gam_send)
    ga_copy.wait()
    gg_copy.wait()


def body(n, m, tv, sv, ta, sa, align, level, step, null, gamma):
    width = tv.shape[-1]
    ta_len = ta.shape[2]
    glevels, heads = gamma.shape
    groups = GROUPS
    window = SLOTS * ta_len
    keys = VB + window
    any_spec = pl.BlockSpec(memory_space=pl.ANY)
    smem = pl.BlockSpec(memory_space=pltpu.SMEM)
    piece = pltpu.VMEM((2, ta_len, width), BF16)
    dma = pltpu.SemaphoreType.DMA
    return pl.pallas_call(
        functools.partial(kernel, n, m, groups, heads),
        out_shape=(
            jax.ShapeDtypeStruct(tv.shape, BF16),
            jax.ShapeDtypeStruct(ta.shape, BF16),
            jax.ShapeDtypeStruct(gamma.shape, F32),
        ),
        in_specs=[any_spec] * 4 + [smem] * 5,
        out_specs=(any_spec, any_spec, any_spec),
        scratch_shapes=[
            pltpu.VMEM((4, keys, width), BF16),
            pltpu.VMEM((VB, width), BF16),
            pltpu.VMEM((VB, width), BF16),
            pltpu.VMEM((3, VB, width), BF16),
            piece,
            pltpu.VMEM((2, window, width), BF16),
            pltpu.VMEM((3, 2, ta_len, width), BF16),
            piece, piece, piece, piece, piece, piece,
            pltpu.VMEM((-(-heads // 8) * 8, 128), F32),
            pltpu.VMEM((n, glevels, 128), F32),
            pltpu.VMEM((m, glevels, 128), F32),
            pltpu.VMEM((glevels, heads), F32),
            dma((6,)),
            dma((groups,)),
            dma((groups, 6)),
            dma((groups, SLOTS)),
            dma((groups, 3)),
            dma((groups, 3)),
            dma((groups, 3)),
            dma((groups, 3)),
            dma((2,)),
            dma((2,)),
        ],
        compiler_params=pltpu.CompilerParams(
            collective_id=0, has_side_effects=True, vmem_limit_bytes=48 * 1024 * 1024
        ),
    )(tv, sv, ta, sa, align, level, step, null, gamma)


def solution(mesh):
    return jax.shard_map(
        functools.partial(body, mesh.shape["seq"], mesh.shape["dp"]),
        mesh=mesh,
        in_specs=(
            P("dp", None, "seq", None),
            P("dp", None, "seq", None),
            P("dp", None, "seq", None),
            P("dp", None, "seq", None),
            P("dp", "seq", None),
            P("dp"),
            P("dp"),
            P("dp"),
            P(),
        ),
        out_specs=(P("dp", None, "seq", None), P("dp", None, "seq", None), P()),
        check_vma=False,
    )
```

```python
import functools

import jax
import jax.numpy as jnp
from jax import lax
from jax.experimental import pallas as pl
from jax.experimental.pallas import tpu as pltpu
from jax.sharding import PartitionSpec as P

VB = 128
REACH = 3
SLOTS = 2 * REACH + 1
GROUPS = 4
MESH = pl.DeviceIdType.MESH
F32 = jnp.float32
BF16 = jnp.bfloat16


def dot(a, b, dims):
    return lax.dot_general(a, b, (dims, ((), ())), preferred_element_type=F32)


NT = ((1,), (1,))
NN = ((1,), (0,))
TN = ((0,), (0,))


def kernel(
    n, m, groups, heads,
    tv, sv, ta, sa, align_in, level_in, step_in, null_in, gamma_in,
    gv_out, ga_out, gg_out,
    kv, qt, qs, gv, ga, pb, rp, rr, rd, ru, sdir, sind, suni, tot, gbuf, gbuf2, gout, un, st, ss,
    align, level_ref, step_ref, null_ref, gamma,
    load_sem, out_sem, in_send, in_recv, a_send, a_recv, g_send, g_recv, gam_send, gam_recv,
):
    width = tv.shape[-1]
    ta_len = ta.shape[2]
    hd = width // heads
    hpg = heads // groups
    gw = hpg * hd
    window = SLOTS * ta_len
    keys = VB + window
    scale = hd ** (-0.5)
    pairs = n // 2

    i = lax.axis_index("seq")
    z = lax.axis_index("dp")
    c = i % 2
    p = i // 2
    po = p % 2
    pe = 1 - po
    dirn = 1 - 2 * po
    d = 2 * c - 1
    partner = i - d
    lo_ok = i >= 2
    hi_ok = i + 2 < n
    ut = i + 3 * d
    u_ok = (ut >= 0) & (ut < n)
    u_slot = 6 * c
    relay = ((po == 0) & (p + 2 < pairs)) | ((po == 1) & (p >= 3))
    first_way = c == po
    ind_ok = ((po == 0) & lo_ok) | ((po == 1) & hi_ok)

    def way(g):
        direct_slot = 3 + 2 * dirn
        if g % 2 == 1:
            return direct_slot, 3 - 2 * dirn, i + 4 * dirn, i - 4 * dirn, relay, None
        return (
            jnp.where(first_way, direct_slot, u_slot),
            1 + 4 * c,
            i + 5 * pe - 1 - 3 * c,
            i - 1 - 3 * pe + 5 * c,
            relay & first_way,
            relay & jnp.logical_not(first_way),
        )

    def krows(r):
        return pl.ds(pl.multiple_of(VB + ta_len * r, ta_len), ta_len)

    def prows(r):
        return pl.ds(pl.multiple_of(ta_len * r, ta_len), ta_len)

    def cols(g):
        return pl.ds(g * gw, gw)

    loads = [
        pltpu.make_async_copy(ta.at[0], kv.at[0:2, krows(REACH), :], load_sem.at[0]),
        pltpu.make_async_copy(sa.at[0], kv.at[2:4, krows(REACH), :], load_sem.at[1]),
        pltpu.make_async_copy(tv.at[0, 0], qt, load_sem.at[2]),
        pltpu.make_async_copy(tv.at[0, 1:3], kv.at[0:2, 0:VB, :], load_sem.at[3]),
        pltpu.make_async_copy(sv.at[0, 0], qs, load_sem.at[4]),
        pltpu.make_async_copy(sv.at[0, 1:3], kv.at[2:4, 0:VB, :], load_sem.at[5]),
        pltpu.make_async_copy(align_in, align, load_sem.at[6]),
        pltpu.make_async_copy(level_in, level_ref, load_sem.at[7]),
        pltpu.make_async_copy(step_in, step_ref, load_sem.at[8]),
        pltpu.make_async_copy(null_in, null_ref, load_sem.at[9]),
        pltpu.make_async_copy(gamma_in, gamma, load_sem.at[10]),
    ]
    for load in loads:
        load.start()

    barrier = pltpu.get_barrier_semaphore()

    def greet_seq(k, carry):
        pl.semaphore_signal(barrier, inc=1, device_id={"seq": (i + k) % n}, device_id_type=MESH)
        return carry

    def greet_dp(k, carry):
        pl.semaphore_signal(barrier, inc=1, device_id={"dp": (z + k) % m}, device_id_type=MESH)
        return carry

    lax.fori_loop(1, n, greet_seq, 0)
    lax.fori_loop(1, m, greet_dp, 0)

    def clear(r):
        kv[:, krows(r), :] = jnp.zeros((4, ta_len, width), BF16)

    @pl.when(jnp.logical_not(lo_ok))
    def _():
        clear(1)
        clear(1 - d)

    @pl.when(jnp.logical_not(hi_ok))
    def _():
        clear(5)
        clear(5 - d)

    @pl.when(jnp.logical_not(u_ok))
    def _():
        clear(u_slot)
        ru[...] = jnp.zeros(ru.shape, BF16)

    tot[...] = jnp.zeros(tot.shape, F32)
    pl.semaphore_wait(barrier, (n - 1) + (m - 1))
    loads[0].wait()
    loads[1].wait()
    for load in loads[6:]:
        load.wait()

    def in_copy(g, kind, src, dst, dev):
        return pltpu.make_async_remote_copy(
            src_ref=kv.at[:, krows(src), cols(g)],
            dst_ref=kv.at[:, krows(dst), cols(g)],
            send_sem=in_send.at[g, kind],
            recv_sem=in_recv.at[g, dst],
            device_id={"seq": dev},
            device_id_type=MESH,
        )

    def in_wait(g, r):
        ref = kv.at[:, krows(r), cols(g)]
        pltpu.make_async_copy(ref, ref, in_recv.at[g, r]).wait()

    def in_sends(g):
        relay_slot, relay_dst, relay_dev = way(g)[:3]
        return (
            (in_copy(g, 0, REACH, 3 - 2 * dirn, i + 2 * dirn), None),
            (in_copy(g, 1, REACH, 3 - 3 * d, ut), u_ok),
            (in_copy(g, 2, REACH, 3 + d, partner), None),
            (in_copy(g, 3, relay_slot, relay_dst, relay_dev), relay),
            (in_copy(g, 4, 1, 1 + d, partner), lo_ok),
            (in_copy(g, 5, 5, 5 + d, partner), hi_ok),
        )

    def guarded(cond, act):
        if cond is None:
            act()
        else:
            pl.when(cond)(act)

    def own(g):
        for copy, cond in in_sends(g)[:3]:
            guarded(cond, copy.start)

    def forward(g):
        guarded(lo_ok, lambda: in_wait(g, 1))
        guarded(hi_ok, lambda: in_wait(g, 5))
        guarded(u_ok, lambda: in_wait(g, u_slot))
        for copy, cond in in_sends(g)[3:]:
            guarded(cond, copy.start)

    level = level_ref[0]
    weight = 1.0 + 0.75 * level.astype(F32)
    loss_weight = 1.0 / (1.0 + jnp.full((1, hd), step_ref[0], jnp.int32).astype(F32) / 250.0)
    first = align[0, 0, 0]
    count = align[0, 0, 1]
    keep = null_ref[0]
    kcol = lax.broadcasted_iota(jnp.int32, (VB, keys), 1)
    owner = i - REACH + (kcol - VB) // ta_len
    usable = (kcol < VB) | ((owner >= first) & (owner < first + count) & (keep == 0))

    def softmax(s):
        e = jnp.exp(s - jnp.max(s, axis=-1, keepdims=True))
        return e * (1.0 / jnp.sum(e, axis=-1, keepdims=True))

    def head_local(h):
        hc = pl.ds(h * hd, hd)
        sc = pl.ds(h * VB, VB)
        s = dot(qt[:, hc], kv[0, :VB, hc], NT) * scale
        st[:, sc] = s
        un[:, hc] = dot(softmax(s).astype(BF16), kv[1, :VB, hc], NN)
        ss[:, sc] = dot(qs[:, hc], kv[2, :VB, hc], NT) * scale

    def head(h):
        hc = pl.ds(h * hd, hd)
        sc = pl.ds(h * VB, VB)
        v = kv[1, :, hc]
        s = dot(qt[:, hc], kv[0, VB:, hc], NT) * scale
        s = jnp.concatenate([st[:, sc], s], axis=1)
        cond = dot(softmax(jnp.where(usable, s, -jnp.inf)).astype(BF16), v, NN)
        unc = un[:, hc]
        target = unc + weight * (cond - unc)
        k = kv[2, :, hc]
        v = kv[3, :, hc]
        q = qs[:, hc]
        s = jnp.concatenate([ss[:, sc], dot(q, k[VB:], NT) * scale], axis=1)
        probs = softmax(jnp.where(usable, s, -jnp.inf))
        pround = probs.astype(BF16)
        out = dot(pround, v, NN)
        factor = gamma[level, h]
        residual = loss_weight * (out * factor - target)
        tot[h : h + 1, :] = jnp.sum(residual * out, axis=0, keepdims=True)
        og = (residual * factor).astype(BF16)
        pg = dot(og, v, NT)
        delta = jnp.sum(og.astype(F32) * out, axis=-1, keepdims=True)
        sg = (scale * probs * (pg - delta)).astype(BF16)
        gv[0, :, hc] = dot(sg, k, NN).astype(BF16)
        kg = dot(sg, q, TN).astype(BF16)
        vg = dot(pround, og, TN).astype(BF16)
        gv[1, :, hc] = kg[:VB]
        gv[2, :, hc] = vg[:VB]
        pb[0, :, hc] = kg[VB:]
        pb[1, :, hc] = vg[VB:]

    def gv_copy(g):
        return pltpu.make_async_copy(gv.at[:, :, cols(g)], gv_out.at[0, :, :, cols(g)], out_sem.at[g])

    def compute(g):
        in_wait(g, 3 - d)
        guarded(lo_ok, lambda: in_wait(g, 1 - d))
        guarded(hi_ok, lambda: in_wait(g, 5 - d))
        for h in range(g * hpg, (g + 1) * hpg):
            head(h)
        gv_copy(g).start()

    base = 1 - d

    def a_copies(g):
        return [
            pltpu.make_async_remote_copy(
                src_ref=pb.at[:, prows(base + 2 * k), cols(g)],
                dst_ref=rp.at[k, :, :, cols(g)],
                send_sem=a_send.at[g, k],
                recv_sem=a_recv.at[g, k],
                device_id={"seq": partner},
                device_id_type=MESH,
            )
            for k in range(3)
        ]

    def stage_a(g):
        for copy in a_copies(g):
            copy.start()

    def g_copy(g, kind, src, dst, dev):
        return pltpu.make_async_remote_copy(
            src_ref=src,
            dst_ref=dst.at[:, :, cols(g)],
            send_sem=g_send.at[g, kind],
            recv_sem=g_recv.at[g, kind],
            device_id={"seq": dev},
            device_id_type=MESH,
        )

    def dir_copy(g):
        return g_copy(g, 0, sdir.at[:, :, cols(g)], rd, i + 2 * dirn)

    def uni_copy(g):
        return g_copy(g, 1, suni.at[:, :, cols(g)], ru, ut)

    def uni_plain(g):
        return g_copy(g, 1, pb.at[:, prows(u_slot), cols(g)], ru, ut)

    def ind_copy(g):
        return g_copy(g, 2, sind.at[:, :, cols(g)], rr, way(g)[3])

    def stage_b(g):
        for copy in a_copies(g):
            copy.wait_recv()
        cs = cols(g)

        @pl.when(ind_ok)
        def _():
            sind[:, :, cs] = (
                pb[:, prows(3 - 2 * dirn), cs].astype(F32) + rp[1 - dirn, :, :, cs].astype(F32)
            ).astype(BF16)
            ind_copy(g).start()

        aff_dir, aff_uni = way(g)[4:]
        plain = u_ok if aff_uni is None else u_ok & jnp.logical_not(aff_uni)
        pl.when(plain)(uni_plain(g).start)

        @pl.when(jnp.logical_not(aff_dir))
        def _():
            sdir[:, :, cs] = (
                pb[:, prows(3 + 2 * dirn), cs].astype(F32) + rp[1 + dirn, :, :, cs].astype(F32)
            ).astype(BF16)
            dir_copy(g).start()

    def stage_c(g):
        cs = cols(g)
        aff_dir, aff_uni = way(g)[4:]
        pl.when(relay)(lambda: ind_copy(g).wait_recv())

        @pl.when(aff_dir)
        def _():
            sdir[:, :, cs] = (
                pb[:, prows(3 + 2 * dirn), cs].astype(F32)
                + rp[1 + dirn, :, :, cs].astype(F32)
                + rr[:, :, cs].astype(F32)
            ).astype(BF16)
            dir_copy(g).start()

        if aff_uni is None:
            return

        @pl.when(aff_uni)
        def _():
            suni[:, :, cs] = (
                pb[:, prows(u_slot), cs].astype(F32) + rr[:, :, cs].astype(F32)
            ).astype(BF16)
            uni_copy(g).start()

    def stage_d(g):
        cs = cols(g)
        dir_copy(g).wait_recv()
        pl.when(u_ok)(lambda: uni_copy(g).wait_recv())
        ga[:, :, cs] = (
            pb[:, prows(REACH), cs].astype(F32)
            + rp[1, :, :, cs].astype(F32)
            + rd[:, :, cs].astype(F32)
            + ru[:, :, cs].astype(F32)
        ).astype(BF16)

    def gam_exchange(buf, which, size, me, axis):
        def send(k, carry):
            pltpu.make_async_remote_copy(
                src_ref=buf.at[me],
                dst_ref=buf.at[me],
                send_sem=gam_send.at[which],
                recv_sem=gam_recv.at[which],
                device_id={axis: (me + k) % size},
                device_id_type=MESH,
            ).start()
            return carry

        lax.fori_loop(1, size, send, 0)

    def gam_wait(buf, which, size, sem):
        ref = buf.at[0 : size - 1]
        pltpu.make_async_copy(ref, ref, sem.at[which]).wait()

    def gamma_first():
        sums = jnp.sum(tot[...], axis=-1, keepdims=True)
        rows = lax.broadcasted_iota(jnp.int32, tot.shape, 0)
        lanes = lax.broadcasted_iota(jnp.int32, tot.shape, 1)
        vec = jnp.sum(jnp.where(rows == lanes, sums, 0.0), axis=0, keepdims=True)
        vec = vec / (VB * n * hd)
        levels = lax.broadcasted_iota(jnp.int32, gbuf.shape[1:], 0)
        gbuf[i] = jnp.where(levels == level, vec, 0.0)
        gam_exchange(gbuf, 0, n, i, "seq")

    def gamma_second():
        gam_wait(gbuf, 0, n, gam_recv)
        gbuf2[z] = jnp.sum(gbuf[...], axis=0)
        gam_exchange(gbuf2, 1, m, z, "dp")

    def gamma_last():
        gam_wait(gbuf2, 1, m, gam_recv)
        gout[...] = jnp.sum(gbuf2[...], axis=0)[:, : gout.shape[1]]

    own(0)
    for load in loads[2:6]:
        load.wait()
    for t in range(groups + 4):
        if t + 1 < groups:
            own(t + 1)
        if t == 0:
            for h in range(heads):
                head_local(h)
        if t < groups:
            forward(t)
        if 0 <= t - 1 < groups:
            compute(t - 1)
            stage_a(t - 1)
            if t - 1 == groups - 1:
                gamma_first()
        if 0 <= t - 2 < groups:
            stage_b(t - 2)
        if t == groups + 2:
            gamma_second()
        if 0 <= t - 3 < groups:
            stage_c(t - 3)
        if 0 <= t - 4 < groups:
            stage_d(t - 4)
    ga_copy = pltpu.make_async_copy(ga, ga_out.at[0], load_sem.at[0])
    ga_copy.start()
    gamma_last()
    gg_copy = pltpu.make_async_copy(gout, gg_out, load_sem.at[1])
    gg_copy.start()
    for g in range(groups):
        gv_copy(g).wait()
        for copy, cond in in_sends(g):
            guarded(cond, copy.wait_send)
        for copy in a_copies(g):
            copy.wait_send()
        dir_copy(g).wait_send()
        pl.when(u_ok)(lambda: uni_copy(g).wait_send())
        pl.when(ind_ok)(lambda: ind_copy(g).wait_send())
    gam_wait(gbuf, 0, n, gam_send)
    gam_wait(gbuf2, 1, m, gam_send)
    ga_copy.wait()
    gg_copy.wait()


def body(n, m, tv, sv, ta, sa, align, level, step, null, gamma):
    width = tv.shape[-1]
    ta_len = ta.shape[2]
    glevels, heads = gamma.shape
    groups = GROUPS
    window = SLOTS * ta_len
    keys = VB + window
    any_spec = pl.BlockSpec(memory_space=pl.ANY)
    hbm_spec = pl.BlockSpec(memory_space=pltpu.HBM)
    piece = pltpu.VMEM((2, ta_len, width), BF16)
    dma = pltpu.SemaphoreType.DMA
    return pl.pallas_call(
        functools.partial(kernel, n, m, groups, heads),
        out_shape=(
            jax.ShapeDtypeStruct(tv.shape, BF16),
            jax.ShapeDtypeStruct(ta.shape, BF16),
            jax.ShapeDtypeStruct(gamma.shape, F32),
        ),
        in_specs=[hbm_spec] * 9,
        out_specs=(any_spec, any_spec, any_spec),
        scratch_shapes=[
            pltpu.VMEM((4, keys, width), BF16),
            pltpu.VMEM((VB, width), BF16),
            pltpu.VMEM((VB, width), BF16),
            pltpu.VMEM((3, VB, width), BF16),
            piece,
            pltpu.VMEM((2, window, width), BF16),
            pltpu.VMEM((3, 2, ta_len, width), BF16),
            piece, piece, piece, piece, piece, piece,
            pltpu.VMEM((-(-heads // 8) * 8, 128), F32),
            pltpu.VMEM((n, glevels, 128), F32),
            pltpu.VMEM((m, glevels, 128), F32),
            pltpu.VMEM((glevels, heads), F32),
            pltpu.VMEM((VB, width), F32),
            pltpu.VMEM((VB, heads * VB), F32),
            pltpu.VMEM((VB, heads * VB), F32),
            pltpu.SMEM(align.shape, jnp.int32),
            pltpu.SMEM(level.shape, jnp.int32),
            pltpu.SMEM(step.shape, jnp.int32),
            pltpu.SMEM(null.shape, jnp.int32),
            pltpu.SMEM(gamma.shape, F32),
            dma((11,)),
            dma((groups,)),
            dma((groups, 6)),
            dma((groups, SLOTS)),
            dma((groups, 3)),
            dma((groups, 3)),
            dma((groups, 3)),
            dma((groups, 3)),
            dma((2,)),
            dma((2,)),
        ],
        compiler_params=pltpu.CompilerParams(
            collective_id=0, has_side_effects=True
        ),
    )(tv, sv, ta, sa, align, level, step, null, gamma)


def solution(mesh):
    return jax.shard_map(
        functools.partial(body, mesh.shape["seq"], mesh.shape["dp"]),
        mesh=mesh,
        in_specs=(
            P("dp", None, "seq", None),
            P("dp", None, "seq", None),
            P("dp", None, "seq", None),
            P("dp", None, "seq", None),
            P("dp", "seq", None),
            P("dp"),
            P("dp"),
            P("dp"),
            P(),
        ),
        out_specs=(P("dp", None, "seq", None), P("dp", None, "seq", None), P()),
        check_vma=False,
    )
```

```python
import functools

import jax
import jax.numpy as jnp
from jax import lax
from jax.experimental import pallas as pl
from jax.experimental.pallas import tpu as pltpu
from jax.sharding import PartitionSpec as P

VB = 128
REACH = 3
SLOTS = 2 * REACH + 1
GROUPS = 4
MESH = pl.DeviceIdType.MESH
F32 = jnp.float32
BF16 = jnp.bfloat16


def dot(a, b, dims):
    return lax.dot_general(a, b, (dims, ((), ())), preferred_element_type=F32)


NT = ((1,), (1,))
NN = ((1,), (0,))
TN = ((0,), (0,))


def kernel(
    n, m, groups, heads,
    tv, sv, ta, sa, align_in, level_in, step_in, null_in, gamma_in,
    gv_out, ga_out, gg_out,
    kv, qt, qs, gv, ga, pb, rp, rr, rd, ru, sdir, sind, suni, tot, gbuf, gbuf2, gout, un, st, ss,
    align, level_ref, step_ref, null_ref, gamma,
    load_sem, out_sem, in_send, in_recv, a_send, a_recv, g_send, g_recv, gam_send, gam_recv,
):
    width = tv.shape[-1]
    ta_len = ta.shape[2]
    hd = width // heads
    hpg = heads // groups
    gw = hpg * hd
    window = SLOTS * ta_len
    keys = VB + window
    scale = hd ** (-0.5)
    pairs = n // 2

    i = lax.axis_index("seq")
    z = lax.axis_index("dp")
    c = i % 2
    p = i // 2
    po = p % 2
    pe = 1 - po
    dirn = 1 - 2 * po
    d = 2 * c - 1
    partner = i - d
    lo_ok = i >= 2
    hi_ok = i + 2 < n
    ut = i + 3 * d
    u_ok = (ut >= 0) & (ut < n)
    u_slot = 6 * c
    relay = ((po == 0) & (p + 2 < pairs)) | ((po == 1) & (p >= 3))
    first_way = c == po
    ind_ok = ((po == 0) & lo_ok) | ((po == 1) & hi_ok)

    def way(g):
        direct_slot = 3 + 2 * dirn
        if g % 2 == 1:
            return direct_slot, 3 - 2 * dirn, i + 4 * dirn, i - 4 * dirn, relay, None
        return (
            jnp.where(first_way, direct_slot, u_slot),
            1 + 4 * c,
            i + 5 * pe - 1 - 3 * c,
            i - 1 - 3 * pe + 5 * c,
            relay & first_way,
            relay & jnp.logical_not(first_way),
        )

    def krows(r):
        return pl.ds(pl.multiple_of(VB + ta_len * r, ta_len), ta_len)

    def prows(r):
        return pl.ds(pl.multiple_of(ta_len * r, ta_len), ta_len)

    def cols(g):
        return pl.ds(g * gw, gw)

    loads = [
        pltpu.make_async_copy(ta.at[0], kv.at[0:2, krows(REACH), :], load_sem.at[0]),
        pltpu.make_async_copy(sa.at[0], kv.at[2:4, krows(REACH), :], load_sem.at[1]),
        pltpu.make_async_copy(tv.at[0, 0], qt, load_sem.at[2]),
        pltpu.make_async_copy(tv.at[0, 1:3], kv.at[0:2, 0:VB, :], load_sem.at[3]),
        pltpu.make_async_copy(sv.at[0, 0], qs, load_sem.at[4]),
        pltpu.make_async_copy(sv.at[0, 1:3], kv.at[2:4, 0:VB, :], load_sem.at[5]),
        pltpu.make_async_copy(align_in, align, load_sem.at[6]),
        pltpu.make_async_copy(level_in, level_ref, load_sem.at[7]),
        pltpu.make_async_copy(step_in, step_ref, load_sem.at[8]),
        pltpu.make_async_copy(null_in, null_ref, load_sem.at[9]),
        pltpu.make_async_copy(gamma_in, gamma, load_sem.at[10]),
    ]
    for load in loads:
        load.start()

    barrier = pltpu.get_barrier_semaphore()

    def greet_seq(k, carry):
        pl.semaphore_signal(barrier, inc=1, device_id={"seq": (i + k) % n}, device_id_type=MESH)
        return carry

    def greet_dp(k, carry):
        pl.semaphore_signal(barrier, inc=1, device_id={"dp": (z + k) % m}, device_id_type=MESH)
        return carry

    lax.fori_loop(1, n, greet_seq, 0)
    lax.fori_loop(1, m, greet_dp, 0)

    def clear(r):
        kv[:, krows(r), :] = jnp.zeros((4, ta_len, width), BF16)

    @pl.when(jnp.logical_not(lo_ok))
    def _():
        clear(1)
        clear(1 - d)

    @pl.when(jnp.logical_not(hi_ok))
    def _():
        clear(5)
        clear(5 - d)

    @pl.when(jnp.logical_not(u_ok))
    def _():
        clear(u_slot)
        ru[...] = jnp.zeros(ru.shape, BF16)

    tot[...] = jnp.zeros(tot.shape, F32)
    pl.semaphore_wait(barrier, (n - 1) + (m - 1))
    loads[0].wait()
    loads[1].wait()
    for load in loads[6:]:
        load.wait()

    def in_copy(g, kind, src, dst, dev):
        return pltpu.make_async_remote_copy(
            src_ref=kv.at[:, krows(src), cols(g)],
            dst_ref=kv.at[:, krows(dst), cols(g)],
            send_sem=in_send.at[g, kind],
            recv_sem=in_recv.at[g, dst],
            device_id={"seq": dev},
            device_id_type=MESH,
        )

    def in_wait(g, r):
        ref = kv.at[:, krows(r), cols(g)]
        pltpu.make_async_copy(ref, ref, in_recv.at[g, r]).wait()

    def in_sends(g):
        relay_slot, relay_dst, relay_dev = way(g)[:3]
        return (
            (in_copy(g, 0, REACH, 3 - 2 * dirn, i + 2 * dirn), None),
            (in_copy(g, 1, REACH, 3 - 3 * d, ut), u_ok),
            (in_copy(g, 2, REACH, 3 + d, partner), None),
            (in_copy(g, 3, relay_slot, relay_dst, relay_dev), relay),
            (in_copy(g, 4, 1, 1 + d, partner), lo_ok),
            (in_copy(g, 5, 5, 5 + d, partner), hi_ok),
        )

    def guarded(cond, act):
        if cond is None:
            act()
        else:
            pl.when(cond)(act)

    def own(g):
        for copy, cond in in_sends(g)[:3]:
            guarded(cond, copy.start)

    def forward(g):
        guarded(u_ok, lambda: in_wait(g, u_slot))
        relayed, low, high = in_sends(g)[3:]

        def pass_low():
            in_wait(g, 1)
            low[0].start()

        def pass_high():
            in_wait(g, 5)
            high[0].start()

        @pl.when(po == 0)
        def _():
            guarded(hi_ok, pass_high)
            guarded(relayed[1], relayed[0].start)
            guarded(lo_ok, pass_low)

        @pl.when(po == 1)
        def _():
            guarded(lo_ok, pass_low)
            guarded(relayed[1], relayed[0].start)
            guarded(hi_ok, pass_high)

    level = level_ref[0]
    weight = 1.0 + 0.75 * level.astype(F32)
    loss_weight = 1.0 / (1.0 + jnp.full((1, hd), step_ref[0], jnp.int32).astype(F32) / 250.0)
    first = align[0, 0, 0]
    count = align[0, 0, 1]
    keep = null_ref[0]
    kcol = lax.broadcasted_iota(jnp.int32, (VB, keys), 1)
    owner = i - REACH + (kcol - VB) // ta_len
    usable = (kcol < VB) | ((owner >= first) & (owner < first + count) & (keep == 0))

    def softmax(s):
        e = jnp.exp(s - jnp.max(s, axis=-1, keepdims=True))
        return e * (1.0 / jnp.sum(e, axis=-1, keepdims=True))

    def head_local(h):
        hc = pl.ds(h * hd, hd)
        sc = pl.ds(h * VB, VB)
        s = dot(qt[:, hc], kv[0, :VB, hc], NT) * scale
        st[:, sc] = s
        un[:, hc] = dot(softmax(s).astype(BF16), kv[1, :VB, hc], NN)
        ss[:, sc] = dot(qs[:, hc], kv[2, :VB, hc], NT) * scale

    def head(h):
        hc = pl.ds(h * hd, hd)
        sc = pl.ds(h * VB, VB)
        v = kv[1, :, hc]
        s = dot(qt[:, hc], kv[0, VB:, hc], NT) * scale
        s = jnp.concatenate([st[:, sc], s], axis=1)
        cond = dot(softmax(jnp.where(usable, s, -jnp.inf)).astype(BF16), v, NN)
        unc = un[:, hc]
        target = unc + weight * (cond - unc)
        k = kv[2, :, hc]
        v = kv[3, :, hc]
        q = qs[:, hc]
        s = jnp.concatenate([ss[:, sc], dot(q, k[VB:], NT) * scale], axis=1)
        probs = softmax(jnp.where(usable, s, -jnp.inf))
        pround = probs.astype(BF16)
        out = dot(pround, v, NN)
        factor = gamma[level, h]
        residual = loss_weight * (out * factor - target)
        tot[h : h + 1, :] = jnp.sum(residual * out, axis=0, keepdims=True)
        og = (residual * factor).astype(BF16)
        pg = dot(og, v, NT)
        delta = jnp.sum(og.astype(F32) * out, axis=-1, keepdims=True)
        sg = (scale * probs * (pg - delta)).astype(BF16)
        gv[0, :, hc] = dot(sg, k, NN).astype(BF16)
        kg = dot(sg, q, TN).astype(BF16)
        vg = dot(pround, og, TN).astype(BF16)
        gv[1, :, hc] = kg[:VB]
        gv[2, :, hc] = vg[:VB]
        pb[0, :, hc] = kg[VB:]
        pb[1, :, hc] = vg[VB:]

    def gv_copy(g):
        return pltpu.make_async_copy(gv.at[:, :, cols(g)], gv_out.at[0, :, :, cols(g)], out_sem.at[g])

    def compute(g):
        in_wait(g, 3 - d)
        guarded(lo_ok, lambda: in_wait(g, 1 - d))
        guarded(hi_ok, lambda: in_wait(g, 5 - d))
        for h in range(g * hpg, (g + 1) * hpg):
            head(h)
        gv_copy(g).start()

    base = 1 - d

    def a_copies(g):
        return [
            pltpu.make_async_remote_copy(
                src_ref=pb.at[:, prows(base + 2 * k), cols(g)],
                dst_ref=rp.at[k, :, :, cols(g)],
                send_sem=a_send.at[g, k],
                recv_sem=a_recv.at[g, k],
                device_id={"seq": partner},
                device_id_type=MESH,
            )
            for k in range(3)
        ]

    def stage_a(g):
        for copy in a_copies(g):
            copy.start()

    def g_copy(g, kind, src, dst, dev):
        return pltpu.make_async_remote_copy(
            src_ref=src,
            dst_ref=dst.at[:, :, cols(g)],
            send_sem=g_send.at[g, kind],
            recv_sem=g_recv.at[g, kind],
            device_id={"seq": dev},
            device_id_type=MESH,
        )

    def dir_copy(g):
        return g_copy(g, 0, sdir.at[:, :, cols(g)], rd, i + 2 * dirn)

    def uni_copy(g):
        return g_copy(g, 1, suni.at[:, :, cols(g)], ru, ut)

    def uni_plain(g):
        return g_copy(g, 1, pb.at[:, prows(u_slot), cols(g)], ru, ut)

    def ind_copy(g):
        return g_copy(g, 2, sind.at[:, :, cols(g)], rr, way(g)[3])

    def stage_b(g):
        for copy in a_copies(g):
            copy.wait_recv()
        cs = cols(g)

        @pl.when(ind_ok)
        def _():
            sind[:, :, cs] = (
                pb[:, prows(3 - 2 * dirn), cs].astype(F32) + rp[1 - dirn, :, :, cs].astype(F32)
            ).astype(BF16)
            ind_copy(g).start()

        aff_dir, aff_uni = way(g)[4:]
        plain = u_ok if aff_uni is None else u_ok & jnp.logical_not(aff_uni)
        pl.when(plain)(uni_plain(g).start)

        @pl.when(jnp.logical_not(aff_dir))
        def _():
            sdir[:, :, cs] = (
                pb[:, prows(3 + 2 * dirn), cs].astype(F32) + rp[1 + dirn, :, :, cs].astype(F32)
            ).astype(BF16)
            dir_copy(g).start()

    def stage_c(g):
        cs = cols(g)
        aff_dir, aff_uni = way(g)[4:]
        pl.when(relay)(lambda: ind_copy(g).wait_recv())

        @pl.when(aff_dir)
        def _():
            sdir[:, :, cs] = (
                pb[:, prows(3 + 2 * dirn), cs].astype(F32)
                + rp[1 + dirn, :, :, cs].astype(F32)
                + rr[:, :, cs].astype(F32)
            ).astype(BF16)
            dir_copy(g).start()

        if aff_uni is None:
            return

        @pl.when(aff_uni)
        def _():
            suni[:, :, cs] = (
                pb[:, prows(u_slot), cs].astype(F32) + rr[:, :, cs].astype(F32)
            ).astype(BF16)
            uni_copy(g).start()

    def stage_d(g):
        cs = cols(g)
        dir_copy(g).wait_recv()
        pl.when(u_ok)(lambda: uni_copy(g).wait_recv())
        ga[:, :, cs] = (
            pb[:, prows(REACH), cs].astype(F32)
            + rp[1, :, :, cs].astype(F32)
            + rd[:, :, cs].astype(F32)
            + ru[:, :, cs].astype(F32)
        ).astype(BF16)

    def gam_exchange(buf, which, size, me, axis):
        def send(k, carry):
            pltpu.make_async_remote_copy(
                src_ref=buf.at[me],
                dst_ref=buf.at[me],
                send_sem=gam_send.at[which],
                recv_sem=gam_recv.at[which],
                device_id={axis: (me + k) % size},
                device_id_type=MESH,
            ).start()
            return carry

        lax.fori_loop(1, size, send, 0)

    def gam_wait(buf, which, size, sem):
        ref = buf.at[0 : size - 1]
        pltpu.make_async_copy(ref, ref, sem.at[which]).wait()

    def gamma_first():
        sums = jnp.sum(tot[...], axis=-1, keepdims=True)
        rows = lax.broadcasted_iota(jnp.int32, tot.shape, 0)
        lanes = lax.broadcasted_iota(jnp.int32, tot.shape, 1)
        vec = jnp.sum(jnp.where(rows == lanes, sums, 0.0), axis=0, keepdims=True)
        vec = vec / (VB * n * hd)
        levels = lax.broadcasted_iota(jnp.int32, gbuf.shape[1:], 0)
        gbuf[i] = jnp.where(levels == level, vec, 0.0)
        gam_exchange(gbuf, 0, n, i, "seq")

    def gamma_second():
        gam_wait(gbuf, 0, n, gam_recv)
        gbuf2[z] = jnp.sum(gbuf[...], axis=0)
        gam_exchange(gbuf2, 1, m, z, "dp")

    def gamma_last():
        gam_wait(gbuf2, 1, m, gam_recv)
        gout[...] = jnp.sum(gbuf2[...], axis=0)[:, : gout.shape[1]]

    for g in range(groups):
        own(g)
    for load in loads[2:6]:
        load.wait()
    for t in range(groups + 4):
        if t == 0:
            for h in range(heads):
                head_local(h)
        if t < groups:
            forward(t)
        if 0 <= t - 1 < groups:
            compute(t - 1)
            stage_a(t - 1)
            if t - 1 == groups - 1:
                gamma_first()
        if 0 <= t - 2 < groups:
            stage_b(t - 2)
        if t == groups + 2:
            gamma_second()
        if 0 <= t - 3 < groups:
            stage_c(t - 3)
        if 0 <= t - 4 < groups:
            stage_d(t - 4)
    ga_copy = pltpu.make_async_copy(ga, ga_out.at[0], load_sem.at[0])
    ga_copy.start()
    gamma_last()
    gg_copy = pltpu.make_async_copy(gout, gg_out, load_sem.at[1])
    gg_copy.start()
    for g in range(groups):
        gv_copy(g).wait()
        for copy, cond in in_sends(g):
            guarded(cond, copy.wait_send)
        for copy in a_copies(g):
            copy.wait_send()
        dir_copy(g).wait_send()
        pl.when(u_ok)(lambda: uni_copy(g).wait_send())
        pl.when(ind_ok)(lambda: ind_copy(g).wait_send())
    gam_wait(gbuf, 0, n, gam_send)
    gam_wait(gbuf2, 1, m, gam_send)
    ga_copy.wait()
    gg_copy.wait()


def body(n, m, tv, sv, ta, sa, align, level, step, null, gamma):
    width = tv.shape[-1]
    ta_len = ta.shape[2]
    glevels, heads = gamma.shape
    groups = GROUPS
    window = SLOTS * ta_len
    keys = VB + window
    any_spec = pl.BlockSpec(memory_space=pl.ANY)
    hbm_spec = pl.BlockSpec(memory_space=pltpu.HBM)
    piece = pltpu.VMEM((2, ta_len, width), BF16)
    dma = pltpu.SemaphoreType.DMA
    return pl.pallas_call(
        functools.partial(kernel, n, m, groups, heads),
        out_shape=(
            jax.ShapeDtypeStruct(tv.shape, BF16),
            jax.ShapeDtypeStruct(ta.shape, BF16),
            jax.ShapeDtypeStruct(gamma.shape, F32),
        ),
        in_specs=[hbm_spec] * 9,
        out_specs=(any_spec, any_spec, any_spec),
        scratch_shapes=[
            pltpu.VMEM((4, keys, width), BF16),
            pltpu.VMEM((VB, width), BF16),
            pltpu.VMEM((VB, width), BF16),
            pltpu.VMEM((3, VB, width), BF16),
            piece,
            pltpu.VMEM((2, window, width), BF16),
            pltpu.VMEM((3, 2, ta_len, width), BF16),
            piece, piece, piece, piece, piece, piece,
            pltpu.VMEM((-(-heads // 8) * 8, 128), F32),
            pltpu.VMEM((n, glevels, 128), F32),
            pltpu.VMEM((m, glevels, 128), F32),
            pltpu.VMEM((glevels, heads), F32),
            pltpu.VMEM((VB, width), F32),
            pltpu.VMEM((VB, heads * VB), F32),
            pltpu.VMEM((VB, heads * VB), F32),
            pltpu.SMEM(align.shape, jnp.int32),
            pltpu.SMEM(level.shape, jnp.int32),
            pltpu.SMEM(step.shape, jnp.int32),
            pltpu.SMEM(null.shape, jnp.int32),
            pltpu.SMEM(gamma.shape, F32),
            dma((11,)),
            dma((groups,)),
            dma((groups, 6)),
            dma((groups, SLOTS)),
            dma((groups, 3)),
            dma((groups, 3)),
            dma((groups, 3)),
            dma((groups, 3)),
            dma((2,)),
            dma((2,)),
        ],
        compiler_params=pltpu.CompilerParams(
            collective_id=0, has_side_effects=True
        ),
    )(tv, sv, ta, sa, align, level, step, null, gamma)


def solution(mesh):
    return jax.shard_map(
        functools.partial(body, mesh.shape["seq"], mesh.shape["dp"]),
        mesh=mesh,
        in_specs=(
            P("dp", None, "seq", None),
            P("dp", None, "seq", None),
            P("dp", None, "seq", None),
            P("dp", None, "seq", None),
            P("dp", "seq", None),
            P("dp"),
            P("dp"),
            P("dp"),
            P(),
        ),
        out_specs=(P("dp", None, "seq", None), P("dp", None, "seq", None), P()),
        check_vma=False,
    )
```
